32 devices in a mesh: dp: 8 (over y, x, core), pencil: 4 (over z).
Axes of the slice: x: 2, y: 2, z: 4, core: 2. Of those that a mesh axis runs over, the one named last changes fastest.
Arguments:
- field: bfloat16 [8, 64, 64, 64, 128], P('dp', 'pencil'), may hold values from -6 to 6
- cotangent: bfloat16 [8, 64, 64, 64, 128], P('dp', 'pencil'), may hold values from -6 to 6
- w_spec: bfloat16 [16, 16, 16, 64, 128], P('dp', 'pencil'), may hold values from -6 to 6
- w_local: bfloat16 [64, 64], replicated, may hold values from -0.75 to 0.75
Outputs:
- grad_field: bfloat16 [8, 64, 64, 64, 128], P('dp', 'pencil')
- grad_w: float32 [16, 16, 16, 64, 128], P('dp', 'pencil')
The draws below stay inside these ranges and needn't reach their ends.
All inputs are finite; a program needn't handle non-finite values.
Results may differ from the reference program's by a relative error of at most 0.02.
Values may be sent and summed in bfloat16 or wider, within the bound.
No kernel may reach another device: no remote copies, remote signals or barrier semaphores. Data moves between devices by JAX's collectives and lax.ppermute only.
A program may use at most 192 MiB of HBM per device.

```python
import math
import jax
import jax.numpy as jnp
from jax import lax

NX = 64
NY = 64
NZ = 128
CH = 64
MX = 16
MY = 16
MZ = 16
SAMPLES = 8


def block_levels(stream_key, shape, shards, smallest, largest):
    def one(dim, parts):
        draws = jax.random.uniform(jax.random.fold_in(jax.random.fold_in(stream_key, 6), dim), (parts,), jnp.float32, smallest / len(shards), largest / len(shards))
        return jnp.repeat(jnp.exp(draws), shape[dim] // parts).reshape((-1,) + (1,) * (len(shape) - dim - 1))

    level = one(*shards[0])
    for cut in shards[1:]:
        level = level * one(*cut)
    return level


def bell_draw(own_key, shape, scale, bound, cuts=(), kind=jnp.bfloat16):
    entries = jax.random.normal(own_key, shape, jnp.float32) * scale
    if len(cuts) > 0:
        entries = block_levels(own_key, shape, cuts, -0.22, 0.18) * entries
    return jnp.clip(entries, min=-bound, max=bound).astype(kind)


def setup_inputs(seed: int = 0) -> dict:
    arg_keys = jax.random.split(jax.random.key(seed), 5)
    field = bell_draw(arg_keys[0], (SAMPLES, NX, NY, CH, NZ), 1.0, 6.0, ((0, 8), (1, 4)))
    cotangent = bell_draw(arg_keys[1], (SAMPLES, NX, NY, CH, NZ), 1.0, 6.0, ((0, 8), (1, 4)))
    w_spec = bell_draw(arg_keys[2], (MX, MY, MZ, CH, 2 * CH), 1.0, 6.0, ((0, 8), (1, 4)))
    w_local = bell_draw(arg_keys[3], (CH, CH), CH ** -0.5, 0.75)
    return {"field": field, "cotangent": cotangent, "w_spec": w_spec, "w_local": w_local}


HIGHEST = lax.Precision.HIGHEST

def phase_pair(length, mode_count, signed):
    position = jnp.arange(length, dtype=jnp.int32)
    indices = jnp.arange(mode_count, dtype=jnp.int32)
    frequency = jnp.where(indices < mode_count // 2, indices, indices - mode_count) if signed else indices
    product = jnp.mod(position[:, None] * frequency[None, :], length).astype(jnp.float32)
    angles = product * (2.0 * math.pi / length)
    return (jnp.cos(angles), jnp.sin(angles))

def grid_tables():
    cos_x, sin_x = phase_pair(NX, MX, True)
    cos_y, sin_y = phase_pair(NY, MY, True)
    cos_z, sin_z = phase_pair(NZ, MZ, False)
    forward_z = jnp.concatenate([cos_z, -sin_z], 1).astype(jnp.bfloat16)
    weight_z = jnp.where(jnp.arange(MZ, dtype=jnp.int32) == 0, 1.0, 2.0).astype(jnp.float32) / (NX * NY * NZ)
    inverse_z = jnp.concatenate([cos_z * weight_z, -sin_z * weight_z], 1).T
    adjoint_z = jnp.concatenate([cos_z, -sin_z], 1).T
    spectrum_scale = jnp.concatenate([weight_z, weight_z])
    return (cos_x, sin_x, cos_y, sin_y, forward_z, inverse_z, adjoint_z, spectrum_scale)

def rotate_half(values):
    middle = values.shape[-1] // 2
    return jnp.concatenate([values[..., middle:], -values[..., :middle]], -1)

def along_y(values, cosines, sine_table, inverse):
    pattern = 'xjck,yj->xyck' if inverse else 'xyck,yj->xjck'
    factor = -1.0 if inverse else 1.0
    direct = jnp.einsum(pattern, values, cosines, precision=HIGHEST)
    turned = jnp.einsum(pattern, rotate_half(values), sine_table, precision=HIGHEST)
    return direct + factor * turned

def along_x(values, cosines, sine_table, inverse):
    pattern = 'jbck,xj->xbck' if inverse else 'xbck,xj->jbck'
    factor = -1.0 if inverse else 1.0
    direct = jnp.einsum(pattern, values, cosines, precision=HIGHEST)
    turned = jnp.einsum(pattern, rotate_half(values), sine_table, precision=HIGHEST)
    return direct + factor * turned

def z_forward(field_in, matrix):
    shape_in = field_in.shape
    product = jnp.dot(field_in.reshape(-1, shape_in[-1]), matrix, preferred_element_type=jnp.float32)
    return product.reshape(shape_in[:-1] + (matrix.shape[1],))

def z_back(values, matrix):
    shape_in = values.shape
    product = jnp.dot(values.reshape(-1, shape_in[-1]), matrix, precision=HIGHEST, preferred_element_type=jnp.float32)
    return product.reshape(shape_in[:-1] + (matrix.shape[1],))

def gelu_slope(pre):
    normal_cdf = 0.5 * (1.0 + lax.erf(pre * (1.0 / math.sqrt(2.0))))
    return normal_cdf + pre * jnp.exp(-0.5 * pre * pre) * (1.0 / math.sqrt(2.0 * math.pi))

def apply_modes(coeffs, weights):
    real_part = coeffs[..., :MZ]
    imag_part = coeffs[..., MZ:]
    from_real = jnp.einsum('abik,abkio->abok', real_part, weights, precision=HIGHEST)
    from_imag = jnp.einsum('abik,abkio->abok', imag_part, weights, precision=HIGHEST)
    out_real = from_real[:, :, :CH] - from_imag[:, :, CH:]
    out_imag = from_real[:, :, CH:] + from_imag[:, :, :CH]
    return jnp.concatenate([out_real, out_imag], -1)

def paired(g_modes):
    g_real = g_modes[..., :MZ]
    g_imag = g_modes[..., MZ:]
    return (jnp.concatenate([g_real, g_imag], -2), jnp.concatenate([g_imag, -g_real], -2))

def adjoint_modes(g_modes, weights):
    paired_one, paired_two = paired(g_modes)
    back_real = jnp.einsum('abkio,abok->abik', weights, paired_one, precision=HIGHEST)
    back_imag = jnp.einsum('abkio,abok->abik', weights, paired_two, precision=HIGHEST)
    return jnp.concatenate([back_real, back_imag], -1)

def mode_grads(u_modes, g_modes):
    paired_one, paired_two = paired(g_modes)
    from_real = jnp.einsum('abik,abok->abkio', u_modes[..., :MZ], paired_one, precision=HIGHEST)
    from_imag = jnp.einsum('abik,abok->abkio', u_modes[..., MZ:], paired_two, precision=HIGHEST)
    return from_real + from_imag

def reference(field, cotangent, w_spec, w_local):
    cos_x, sin_x, cos_y, sin_y, forward_z, inverse_z, adjoint_z, spectrum_scale = grid_tables()
    w_full = w_spec.astype(jnp.float32)
    w_bypass = w_local.astype(jnp.float32)

    def to_modes(field_in):
        sectioned = along_y(z_forward(field_in, forward_z), cos_y, sin_y, False)
        return along_x(sectioned, cos_x, sin_x, False)

    def to_grid(coeffs, matrix):
        sectioned = along_y(along_x(coeffs, cos_x, sin_x, True), cos_y, sin_y, True)
        return z_back(sectioned, matrix)

    def one_sample(accumulated, pair_in):
        sample, target = pair_in
        u_modes = lax.optimization_barrier(to_modes(sample).astype(jnp.bfloat16)).astype(jnp.float32)
        v_modes = apply_modes(u_modes, w_full)
        values = to_grid(v_modes, inverse_z)
        bypass = jnp.einsum('xycz,co->xyoz', sample.astype(jnp.float32), w_bypass, precision=HIGHEST)
        slope_in = (target.astype(jnp.float32) * gelu_slope(values + bypass)).astype(jnp.bfloat16)
        g_modes = lax.optimization_barrier((to_modes(slope_in) * spectrum_scale).astype(jnp.bfloat16)).astype(jnp.float32)
        accumulated = accumulated + mode_grads(u_modes, g_modes)
        back_modes = adjoint_modes(g_modes, w_full)
        spread = jnp.einsum('xyoz,co->xycz', slope_in.astype(jnp.float32), w_bypass, precision=HIGHEST)
        grad_sample = (to_grid(back_modes, adjoint_z) + spread).astype(jnp.bfloat16)
        return (accumulated, grad_sample)
    initial = jnp.zeros((MX, MY, MZ, CH, 2 * CH), jnp.float32)
    grad_w, grad_field = lax.scan(one_sample, initial, (field, cotangent))
    return (grad_field, grad_w)
```

```python
import functools
import math

import jax
import jax.numpy as jnp
import numpy as np
from jax import lax
from jax.experimental import pallas as pl
from jax.experimental.pallas import tpu as pltpu
from jax.sharding import PartitionSpec as P

F32 = jnp.float32
BF16 = jnp.bfloat16
SUB = 16
LIMIT = 60 * 1024 * 1024


def phases(length, count, signed):
    position = np.arange(length)
    index = np.arange(count)
    freq = np.where(index < count // 2, index, index - count) if signed else index
    angle = np.mod(position[:, None] * freq[None, :], length) * (2.0 * math.pi / length)
    return np.cos(angle), np.sin(angle)


def kron_tables(nx, mx, parts):
    cos_x, sin_x = phases(nx, mx, True)
    eye = np.eye(SUB)
    local = nx // parts
    fwd, inv = [], []
    for p in range(parts):
        c = cos_x[p * local : (p + 1) * local]
        s = sin_x[p * local : (p + 1) * local]
        fwd.append(np.concatenate([np.kron(c.T, eye), np.kron(s.T, eye)], 1))
        inv.append(np.concatenate([np.kron(c, eye), np.kron(s, eye)], 1))
    return np.stack(fwd).astype(jnp.bfloat16), np.stack(inv).astype(jnp.bfloat16)


def grid_tables(ny, my, nz, mz):
    cos_y, sin_y = phases(ny, my, True)
    cos_z, sin_z = phases(nz, mz, False)
    cos_z = cos_z.astype(jnp.bfloat16).astype(np.float32)
    sin_z = sin_z.astype(jnp.bfloat16).astype(np.float32)
    ytab = np.stack([np.repeat(cos_y, mz, 1), np.repeat(sin_y, mz, 1)]).astype(np.float32)
    ztab = np.stack([np.tile(cos_z, (1, my)), np.tile(sin_z, (1, my))]).astype(np.float32)
    return ytab, ztab


def fill_basis(basis, ytab, ztab, yb, nz):
    cz = ztab[0]
    sz = ztab[1]
    for y in range(yb):
        cy = ytab[0, y : y + 1, :]
        sy = ytab[1, y : y + 1, :]
        re = cy * cz - sy * sz
        im = -(sy * cz + cy * sz)
        basis[y * nz : (y + 1) * nz, :] = jnp.concatenate([re, im], 1).astype(BF16)


def x_forward_store(acc, xf, out, mx, modes):
    xl, ch, _ = acc.shape
    groups = ch // SUB
    parts = []
    for g in range(groups):
        a = acc[:, g * SUB : (g + 1) * SUB, :].reshape(xl * SUB, 2 * modes).astype(BF16)
        re = a[:, :modes]
        im = a[:, modes:]
        rhs = jnp.concatenate(
            [jnp.concatenate([re, im], 1), jnp.concatenate([im, -re], 1)], 0
        )
        parts.append(jnp.dot(xf, rhs, preferred_element_type=F32))
    dp, pencil, jo, mo, _ = out.shape
    for j in range(mx):
        rows = slice(j * SUB, (j + 1) * SUB)
        block = jnp.concatenate(
            [part[rows, :modes] for part in parts] + [part[rows, modes:] for part in parts], 0
        )
        turned = block.T.astype(BF16)
        for q in range(pencil):
            out[j // jo, q, j % jo] = turned[q * mo : (q + 1) * mo, :]


def x_inverse_load(spec, turned, xi, half, xl, ch):
    pencil, dp, jo, mo, _ = spec.shape
    mx = dp * jo
    modes = pencil * mo
    for j in range(mx):
        block = jnp.concatenate([spec[q, j // jo, j % jo] for q in range(pencil)], 0)
        turned[j] = block.astype(F32).T.astype(BF16)
    for g in range(ch // SUB):
        re = turned[:, g * SUB : (g + 1) * SUB, :].reshape(mx * SUB, modes)
        im = turned[:, ch + g * SUB : ch + (g + 1) * SUB, :].reshape(mx * SUB, modes)
        rhs = jnp.concatenate(
            [jnp.concatenate([re, im], 1), jnp.concatenate([-im, re], 1)], 0
        )
        b = jnp.dot(xi, rhs, preferred_element_type=F32)
        half[:, g * SUB : (g + 1) * SUB, :] = b.reshape(xl, SUB, 2 * modes).astype(BF16)


def grid_rows(ref, x0, xn, yb):
    ch, nz = ref.shape[2], ref.shape[3]
    return jnp.concatenate(
        [ref[x0 : x0 + xn, y].reshape(xn * ch, nz) for y in range(yb)], 1
    )


def forward_kernel(rank, field, ytab, ztab, xf, out, basis, acc, *, xn):
    xl, yb, ch, nz = field.shape
    modes = ytab.shape[2]
    step = pl.program_id(0)

    @pl.when(step == 0)
    def _():
        acc[...] = jnp.zeros_like(acc)

    fill_basis(basis, ytab, ztab, yb, nz)
    for x0 in range(0, xl, xn):
        part = jnp.dot(grid_rows(field, x0, xn, yb), basis[...], preferred_element_type=F32)
        acc[x0 : x0 + xn] += part.reshape(xn, ch, 2 * modes)

    @pl.when(step == pl.num_programs(0) - 1)
    def _():
        x_forward_store(acc, xf[0], out, xf.shape[1] // SUB, modes)


def slope_kernel(
    rank, spec, field, cot, mix, ytab, ztab, xf, xi, slope, out, basis, acc, turned, half, *, xn
):
    xl, yb, ch, nz = field.shape
    modes = ytab.shape[2]
    step = pl.program_id(0)

    @pl.when(step == 0)
    def _():
        acc[...] = jnp.zeros_like(acc)
        x_inverse_load(spec, turned, xi[0], half, xl, ch)

    fill_basis(basis, ytab, ztab, yb, nz)
    for x0 in range(0, xl, xn):
        rows = half[x0 : x0 + xn].reshape(xn * ch, 2 * modes)
        pre = lax.dot_general(
            rows, basis[...], (((1,), (1,)), ((), ())), preferred_element_type=F32
        )
        pre = pre + jnp.dot(
            mix[...], grid_rows(field, x0, xn, yb), preferred_element_type=F32
        )
        q = pre * (1.0 / math.sqrt(2.0))
        bell = jnp.exp(-(q * q)) * q
        gain = (0.5 + 0.5 * lax.erf(q)) + bell * (1.0 / math.sqrt(math.pi))
        value = (grid_rows(cot, x0, xn, yb).astype(F32) * gain).astype(BF16)
        for y in range(yb):
            slope[x0 : x0 + xn, y] = value[:, y * nz : (y + 1) * nz].reshape(xn, ch, nz)
        part = jnp.dot(value, basis[...], preferred_element_type=F32)
        acc[x0 : x0 + xn] += part.reshape(xn, ch, 2 * modes)

    @pl.when(step == pl.num_programs(0) - 1)
    def _():
        x_forward_store(acc, xf[0], out, xf.shape[1] // SUB, modes)


def inverse_kernel(rank, spec, slope, mix, ytab, ztab, xi, grad, basis, turned, half, *, xn):
    xl, yb, ch, nz = slope.shape
    modes = ytab.shape[2]

    @pl.when(pl.program_id(0) == 0)
    def _():
        x_inverse_load(spec, turned, xi[0], half, xl, ch)

    fill_basis(basis, ytab, ztab, yb, nz)
    for x0 in range(0, xl, xn):
        rows = half[x0 : x0 + xn].reshape(xn * ch, 2 * modes)
        total = lax.dot_general(
            rows, basis[...], (((1,), (1,)), ((), ())), preferred_element_type=F32
        )
        total = total + jnp.dot(
            mix[...], grid_rows(slope, x0, xn, yb), preferred_element_type=F32
        )
        total = total.astype(BF16)
        for y in range(yb):
            grad[x0 : x0 + xn, y] = total[:, y * nz : (y + 1) * nz].reshape(xn, ch, nz)


def other_half(values):
    return pltpu.roll(values, values.shape[-1] // 2, 1)


def gather_partials(received, store, samples, pencil, scale):
    modes = received.shape[1]
    for s in range(samples):
        total = received[s * pencil].astype(F32)
        for p in range(1, pencil):
            total = total + received[s * pencil + p].astype(F32)
        store[s * modes : (s + 1) * modes, :] = (total * scale).astype(BF16).astype(F32)


def mode_scale(modes, lanes, mz, size):
    k = lax.broadcasted_iota(jnp.int32, (modes, lanes), 0) % mz
    return jnp.where(k == 0, 1.0 / size, 2.0 / size).astype(F32)


def apply_kernel(received, weights, uhat, out, store, result, *, samples, pencil, mz, size):
    modes, ch, wide = weights.shape
    gather_partials(received, store, samples, pencil, 1.0)
    uhat[...] = store[...]
    sign = jnp.where(
        lax.broadcasted_iota(jnp.int32, (samples, wide), 1) < ch, -1.0, 1.0
    ).astype(F32)

    def one(m):
        rows = pl.ds(m, samples, stride=modes)
        u = store[rows, :]
        lhs = jnp.concatenate([u, other_half(u)], 0)[:, :ch].astype(BF16)
        both = jnp.dot(lhs, weights[m], preferred_element_type=F32)
        result[rows, :] = both[:samples] + sign * other_half(both[samples:])

    for m in range(modes):
        one(m)
    scale = mode_scale(modes, wide, mz, size)
    for s in range(samples):
        out[s] = (result[s * modes : (s + 1) * modes, :] * scale).astype(BF16)


def adjoint_kernel(
    received, weights, uhat, out, grad, store, result, *, samples, pencil, mz, size, total
):
    block, ch, wide = weights.shape
    step = pl.program_id(0)

    @pl.when(step == 0)
    def _():
        gather_partials(received, store, samples, pencil, mode_scale(total, wide, mz, size))

    low = lax.broadcasted_iota(jnp.int32, (samples, wide), 1) < ch
    sign = jnp.where(low, 1.0, -1.0).astype(F32)
    for i in range(block):
        rows = pl.ds(step * block + i, samples, stride=total)
        u = uhat[rows, :]
        g = store[rows, :]
        uu = jnp.concatenate([u, other_half(u)], 0)[:, :ch].astype(BF16)
        gg = jnp.concatenate([g, sign * other_half(g)], 0).astype(BF16)
        w = weights[i]
        both = lax.dot_general(
            gg, jnp.concatenate([w, w], 0), (((1,), (1,)), ((), ())), preferred_element_type=F32
        )
        result[rows, :] = jnp.where(low, both[:samples], both[samples:])
        grad[i] = lax.dot_general(
            uu, gg, (((0,), (0,)), ((), ())), preferred_element_type=F32
        )

    @pl.when(step == pl.num_programs(0) - 1)
    def _():
        for s in range(samples):
            out[s] = result[s * total : (s + 1) * total, :].astype(BF16)


def params():
    return pltpu.CompilerParams(
        dimension_semantics=("arbitrary",), vmem_limit_bytes=LIMIT
    )


def whole(shape):
    return pl.BlockSpec(shape, lambda i, r: (0,) * len(shape))


def make_body(dp, pencil):
    def body(field, cotangent, w_spec, w_local):
        sample = field[0]
        target = cotangent[0]
        xl, ny, ch, nz = sample.shape
        jo, lo, mz, _, wide = w_spec.shape
        nx, mx, my = xl * pencil, jo * dp, lo * pencil
        modes = my * mz
        mo = lo * mz
        samples = dp
        owned = jo * mo
        size = nx * ny * nz
        xn = min(xl, 4)
        rank = lax.axis_index("pencil").astype(jnp.int32).reshape(1)

        xf, xi = kron_tables(nx, mx, pencil)
        ytab, ztab = grid_tables(ny, my, nz, mz)
        weights = w_spec.reshape(owned, ch, wide)
        mix_out = jnp.kron(jnp.eye(xn, dtype=BF16), w_local.T)
        mix_in = jnp.kron(jnp.eye(xn, dtype=BF16), w_local)

        def grid_spec(yb):
            return pl.BlockSpec((xl, yb, ch, nz), lambda i, r: (0, i, 0, 0))

        def y_spec(yb):
            return pl.BlockSpec((2, None, yb, modes), lambda i, r: (0, i, 0, 0))

        def y_table(yb):
            return ytab.reshape(2, ny // yb, yb, modes)

        z_spec = whole(ztab.shape)
        ranked = lambda t: pl.BlockSpec((1,) + t.shape[1:], lambda i, r: (r[0], 0, 0))
        packed = (dp, pencil, jo, mo, 2 * ch)
        unpacked = (pencil, dp, jo, mo, 2 * ch)

        def call(kernel, yb, ins, outs, shapes, scratch, name, args):
            return pl.pallas_call(
                functools.partial(kernel, xn=xn),
                grid_spec=pltpu.PrefetchScalarGridSpec(
                    num_scalar_prefetch=1,
                    grid=(ny // yb,),
                    in_specs=ins,
                    out_specs=outs,
                    scratch_shapes=scratch,
                ),
                out_shape=shapes,
                compiler_params=params(),
                name=name,
            )(rank, *args)

        def basis(yb):
            return pltpu.VMEM((yb * nz, 2 * modes), BF16)

        acc = pltpu.VMEM((xl, ch, 2 * modes), F32)
        turned = pltpu.VMEM((mx, 2 * ch, modes), BF16)
        half = pltpu.VMEM((xl, ch, 2 * modes), BF16)
        spectrum = jax.ShapeDtypeStruct(packed, BF16)
        grid_shape = jax.ShapeDtypeStruct(sample.shape, BF16)

        def to_owner(values):
            flat = values.reshape((dp * pencil, owned, 2 * ch))
            return lax.all_to_all(flat, ("dp", "pencil"), 0, 0, tiled=True)

        def from_owner(values):
            sent = jnp.broadcast_to(values[:, None], (dp, pencil, owned, 2 * ch))
            got = lax.all_to_all(
                sent.reshape(dp * pencil, owned, 2 * ch), ("dp", "pencil"), 0, 0, tiled=True
            )
            got = got.reshape(dp, pencil, jo, mo, 2 * ch)
            return got.transpose(1, 0, 2, 3, 4)

        yb = 8
        s1 = call(
            forward_kernel,
            yb,
            [grid_spec(yb), y_spec(yb), z_spec, ranked(xf)],
            whole(packed),
            spectrum,
            [basis(yb), acc],
            "field_modes",
            (sample, y_table(yb), ztab, xf),
        )
        u_got = to_owner(s1)
        rows = pltpu.VMEM((samples * owned, 2 * ch), F32)
        sizes = dict(samples=samples, pencil=pencil, mz=mz, size=size)
        uhat, v_own = pl.pallas_call(
            functools.partial(apply_kernel, **sizes),
            out_shape=(
                jax.ShapeDtypeStruct((samples * owned, 2 * ch), F32),
                jax.ShapeDtypeStruct((samples, owned, 2 * ch), BF16),
            ),
            scratch_shapes=[rows, rows],
            compiler_params=pltpu.CompilerParams(vmem_limit_bytes=LIMIT),
            name="apply_modes",
        )(u_got, weights)
        v = from_owner(v_own)
        yb = 4
        slope, s2 = call(
            slope_kernel,
            yb,
            [
                whole(unpacked),
                grid_spec(yb),
                grid_spec(yb),
                whole(mix_out.shape),
                y_spec(yb),
                z_spec,
                ranked(xf),
                ranked(xi),
            ],
            (grid_spec(yb), whole(packed)),
            (grid_shape, spectrum),
            [basis(yb), acc, turned, half],
            "slope_modes",
            (v, sample, target, mix_out, y_table(yb), ztab, xf, xi),
        )
        g_got = to_owner(s2)
        steps = 8 if owned % 8 == 0 else 1
        block = owned // steps
        fixed = lambda shape: pl.BlockSpec(shape, lambda i: (0,) * len(shape))
        moving = pl.BlockSpec((block, ch, wide), lambda i: (i, 0, 0))
        du_own, grad_w = pl.pallas_call(
            functools.partial(adjoint_kernel, total=owned, **sizes),
            grid=(steps,),
            in_specs=[fixed(g_got.shape), moving, fixed(uhat.shape)],
            out_specs=(fixed((samples, owned, 2 * ch)), moving),
            out_shape=(
                jax.ShapeDtypeStruct((samples, owned, 2 * ch), BF16),
                jax.ShapeDtypeStruct((owned, ch, wide), F32),
            ),
            scratch_shapes=[rows, rows],
            compiler_params=params(),
            name="adjoint_modes",
        )(g_got, weights, uhat)
        du = from_owner(du_own)
        grad = call(
            inverse_kernel,
            yb,
            [
                whole(unpacked),
                grid_spec(yb),
                whole(mix_in.shape),
                y_spec(yb),
                z_spec,
                ranked(xi),
            ],
            grid_spec(yb),
            grid_shape,
            [basis(yb), turned, half],
            "grad_field",
            (du, slope, mix_in, y_table(yb), ztab, xi),
        )
        return grad[None], grad_w.reshape(jo, lo, mz, ch, wide)

    return body


def solution(mesh):
    split = P("dp", "pencil", None, None, None)
    return jax.shard_map(
        make_body(mesh.shape["dp"], mesh.shape["pencil"]),
        mesh=mesh,
        in_specs=(split, split, split, P()),
        out_specs=(split, split),
        check_vma=False,
    )
```

```python
import functools
import math

import jax
import jax.numpy as jnp
import numpy as np
from jax import lax
from jax.experimental import pallas as pl
from jax.experimental.pallas import tpu as pltpu
from jax.sharding import PartitionSpec as P

F32 = jnp.float32
BF16 = jnp.bfloat16
SUB = 16
LIMIT = 60 * 1024 * 1024
BELL = 1.0 - 0.5 * math.log2(math.pi)


def phases(length, count, signed):
    position = np.arange(length)
    index = np.arange(count)
    freq = np.where(index < count // 2, index, index - count) if signed else index
    angle = np.mod(position[:, None] * freq[None, :], length) * (2.0 * math.pi / length)
    return np.cos(angle), np.sin(angle)


def kron_tables(nx, mx, parts):
    cos_x, sin_x = phases(nx, mx, True)
    eye = np.eye(SUB)
    local = nx // parts
    fwd, inv = [], []
    for p in range(parts):
        c = cos_x[p * local : (p + 1) * local]
        s = sin_x[p * local : (p + 1) * local]
        fwd.append(np.concatenate([np.kron(c.T, eye), np.kron(s.T, eye)], 1))
        inv.append(np.concatenate([np.kron(c, eye), np.kron(s, eye)], 1))
    return np.stack(fwd).astype(jnp.bfloat16), np.stack(inv).astype(jnp.bfloat16)


HALVES = 2


def grid_tables(ny, my, nz, mz, folded):
    cos_y, sin_y = phases(ny, my, True)
    cos_z, sin_z = phases(nz, mz, False)
    cos_z = cos_z.astype(jnp.bfloat16).astype(np.float32)
    sin_z = sin_z.astype(jnp.bfloat16).astype(np.float32)
    kh = mz // HALVES

    def pick(y, z, t):
        if folded:
            y = y[: ny // HALVES, t::HALVES]
        else:
            z = z[:, t * kh : (t + 1) * kh]
        return np.repeat(y, z.shape[1], 1), np.tile(z, (1, y.shape[1]))

    ytab, ztab = [], []
    for y, z in ((cos_y, cos_z), (sin_y, sin_z)):
        pairs = [pick(y, z, t) for t in range(HALVES)]
        ytab.append([p[0] for p in pairs])
        ztab.append([p[1] for p in pairs])
    return np.array(ytab, np.float32), np.array(ztab, np.float32)


def fill_basis(basis, ytab, ztab, i):
    yb = ytab.shape[3]
    nz = ztab.shape[2]
    for t in range(HALVES):
        cz = ztab[0, t]
        sz = ztab[1, t]
        for y in range(yb):
            cy = ytab[0, t, i, y : y + 1, :]
            sy = ytab[1, t, i, y : y + 1, :]
            re = cy * cz - sy * sz
            im = -(sy * cz + cy * sz)
            basis[t][y * nz : (y + 1) * nz, :] = jnp.concatenate([re, im], 1).astype(BF16)


def x_forward_store(acc, xf, out, mx):
    xl, ch, wide = acc[0].shape
    kept = wide // 2
    parts = []
    for g in range(ch // SUB):
        sides = []
        for t in range(HALVES):
            a = acc[t][:, g * SUB : (g + 1) * SUB, :].reshape(xl * SUB, wide).astype(BF16)
            re = a[:, :kept]
            im = a[:, kept:]
            sides.append(
                jnp.concatenate(
                    [jnp.concatenate([re, im], 1), jnp.concatenate([im, -re], 1)], 0
                )
            )
        rhs = jnp.concatenate(sides, 1)
        parts.append(jnp.dot(xf, rhs, preferred_element_type=F32))
    dp, pencil, jo, mo, _ = out.shape
    for j in range(mx):
        rows = slice(j * SUB, (j + 1) * SUB)
        pieces = [
            part[rows, n * kept : (n + 1) * kept] for n in range(2 * HALVES) for part in parts
        ]
        turned = jnp.concatenate(pieces, 0).T.astype(BF16)
        for q in range(pencil):
            out[j // jo, q, j % jo] = turned[q * mo : (q + 1) * mo, :]


def x_inverse_load(spec, turned, xi, half, jo, pencil):
    xl, ch, wide = half[0].shape
    mx = turned.shape[0]
    mo = spec.shape[1] // jo
    for j in range(mx):
        first = (j // jo) * pencil
        rows = slice((j % jo) * mo, (j % jo + 1) * mo)
        block = jnp.concatenate([spec[first + q, rows] for q in range(pencil)], 0)
        turned[j] = block.astype(F32).T.astype(BF16)
    for g in range(ch // SUB):
        sides = []
        for t in range(HALVES):
            re, im = [
                turned[:, n * ch + g * SUB : n * ch + (g + 1) * SUB, :].reshape(
                    mx * SUB, wide // 2
                )
                for n in (2 * t, 2 * t + 1)
            ]
            sides.append(
                jnp.concatenate(
                    [jnp.concatenate([re, im], 1), jnp.concatenate([-im, re], 1)], 0
                )
            )
        b = jnp.dot(xi, jnp.concatenate(sides, 1), preferred_element_type=F32)
        for t in range(HALVES):
            half[t][:, g * SUB : (g + 1) * SUB, :] = (
                b[:, t * wide : (t + 1) * wide].reshape(xl, SUB, wide).astype(BF16)
            )


def grid_rows(ref, x0, xn, yb):
    ch, nz = ref.shape[2], ref.shape[3]
    return jnp.concatenate(
        [ref[x0 : x0 + xn, y].reshape(xn * ch, nz) for y in range(yb)], 1
    )


def mixed(mix, ref, x0, xn, yb):
    per = mix.shape[1] // ref.shape[2]
    table = mix[...]
    return jnp.concatenate(
        [
            jnp.dot(table, grid_rows(ref, x, per, yb), preferred_element_type=F32)
            for x in range(x0, x0 + xn, per)
        ],
        0,
    )


def forward_sums(values, basis, acc, x0, xn):
    ch = acc[0].shape[1]
    if len(values) == 2:
        sides = (values[0] + values[1], values[0] - values[1])
    else:
        sides = (values[0], values[0])
    for t in range(HALVES):
        part = jnp.dot(sides[t], basis[t][...], preferred_element_type=F32)
        acc[t][x0 : x0 + xn] += part.reshape(xn, ch, part.shape[1])


def inverse_sums(half, basis, x0, xn, count):
    sides = []
    for t in range(HALVES):
        rows = half[t][x0 : x0 + xn]
        rows = rows.reshape(xn * rows.shape[1], rows.shape[2])
        sides.append(
            lax.dot_general(
                rows, basis[t][...], (((1,), (1,)), ((), ())), preferred_element_type=F32
            )
        )
    if count == 2:
        return [sides[0] + sides[1], sides[0] - sides[1]]
    return [sides[0] + sides[1]]


def block_copies(src, dst, sems, row, first):
    _, _, yb, chans, _ = dst.shape

    def one(i):
        return pltpu.make_async_copy(
            src.at[:, pl.ds(i * yb, yb), pl.ds(first, chans)], dst.at[i], sems.at[row, i]
        )

    return one


def step_blocks(i, steps, blocks):
    return [i + n * steps for n in range(blocks // steps)]


AHEAD = 2


def start_first(steps, blocks, loads):
    for i in range(min(AHEAD, steps)):
        for b in step_blocks(i, steps, blocks):
            for load in loads:
                load(b).start()


def start_next(i, steps, blocks, loads):
    @pl.when(i + AHEAD < steps)
    def _():
        for b in step_blocks(i + AHEAD, steps, blocks):
            for load in loads:
                load(b).start()


def forward_kernel(
    rank, field, ytab, ztab, xf, out, b0, b1, a0, a1, fbuf, sems, *, xn, jo, first
):
    basis, acc = (b0, b1), (a0, a1)
    blocks, xl, yb, ch, nz = fbuf.shape
    steps = ytab.shape[2]
    load = block_copies(field, fbuf, sems, 0, first)
    start_first(steps, blocks, [load])
    for part in acc:
        part[...] = jnp.zeros_like(part)

    def step(i, carry):
        fill_basis(basis, ytab, ztab, i)
        held = step_blocks(i, steps, blocks)
        start_next(i, steps, blocks, [load])
        for b in held:
            load(b).wait()
        for x0 in range(0, xl, xn):
            values = [grid_rows(fbuf.at[b], x0, xn, yb) for b in held]
            forward_sums(values, basis, acc, x0, xn)
        return carry

    lax.fori_loop(0, steps, step, 0)
    x_forward_store(acc, xf[0], out, xf.shape[1] // SUB)


def slope_kernel(rank, spec, mix, ytab, ztab, xf, xi, field, cot, *rest, xn, jo, first):
    slope, out, b0, b1, a0, a1, turned, h0, h1, fbuf, cbuf, sems = rest[-12:]
    basis, acc, half = (b0, b1), (a0, a1), (h0, h1)
    blocks, xl, yb, ch, nz = cbuf.shape
    steps = ytab.shape[2]
    load_f = block_copies(field, fbuf, sems, 0, 0)
    load_c = block_copies(cot, cbuf, sems, 1, first)
    start_first(steps, blocks, [load_f, load_c])

    def store(b):
        return pltpu.make_async_copy(
            cbuf.at[b], slope.at[:, pl.ds(b * yb, yb), pl.ds(first, ch)], sems.at[2, b]
        )

    for part in acc:
        part[...] = jnp.zeros_like(part)
    x_inverse_load(spec, turned, xi[0], half, jo, out.shape[1])

    def step(i, carry):
        fill_basis(basis, ytab, ztab, i)
        held = step_blocks(i, steps, blocks)
        start_next(i, steps, blocks, [load_f, load_c])
        for b in held:
            load_f(b).wait()
            load_c(b).wait()
        starts = list(range(0, xl, xn))

        def before(x0):
            grid = inverse_sums(half, basis, x0, xn, len(held))
            return [
                pre + mixed(mix, fbuf.at[b], x0, xn, yb) for b, pre in zip(held, grid)
            ]

        ahead = before(starts[0])
        for n, x0 in enumerate(starts):
            grid = ahead
            if n + 1 < len(starts):
                ahead = before(starts[n + 1])
            values = []
            for b, pre in zip(held, grid):
                cot_b = cbuf.at[b]
                q = pre * (1.0 / math.sqrt(2.0))
                bell = jnp.exp2(q * q * (-math.log2(math.e)) + BELL) * q
                gain = (1.0 + lax.erf(q)) + bell
                value = grid_rows(cot_b, x0, xn, yb) * gain.astype(BF16)
                for y in range(yb):
                    cot_b[x0 : x0 + xn, y] = value[:, y * nz : (y + 1) * nz].reshape(xn, ch, nz)
                values.append(value)
            forward_sums(values, basis, acc, x0, xn)
        for b in held:
            store(b).start()
        return carry

    lax.fori_loop(0, steps, step, 0)
    x_forward_store(acc, xf[0], out, xf.shape[1] // SUB)
    for b in range(blocks):
        store(b).wait()


def inverse_kernel(rank, spec, mix, ytab, ztab, xi, slope, *rest, xn, jo, pencil, first):
    grad, b0, b1, turned, h0, h1, sbuf, gbuf, sems = rest[-9:]
    basis, half = (b0, b1), (h0, h1)
    blocks, xl, yb, ch, nz = gbuf.shape
    steps = ytab.shape[2]
    load = block_copies(slope, sbuf, sems, 0, 0)
    start_first(steps, blocks, [load])

    def store(b):
        return pltpu.make_async_copy(
            gbuf.at[b], grad.at[:, pl.ds(b * yb, yb), pl.ds(first, ch)], sems.at[1, b]
        )

    x_inverse_load(spec, turned, xi[0], half, jo, pencil)

    def step(i, carry):
        fill_basis(basis, ytab, ztab, i)
        held = step_blocks(i, steps, blocks)
        start_next(i, steps, blocks, [load])
        for b in held:
            load(b).wait()
        starts = list(range(0, xl, xn))

        def before(x0):
            grid = inverse_sums(half, basis, x0, xn, len(held))
            return [(mixed(mix, sbuf.at[b], x0, xn, yb), g) for b, g in zip(held, grid)]

        ahead = before(starts[0])
        for n, x0 in enumerate(starts):
            grid = ahead
            if n + 1 < len(starts):
                ahead = before(starts[n + 1])
            for b, (spread, total) in zip(held, grid):
                out_b = gbuf.at[b]
                total = (total + spread).astype(BF16)
                for y in range(yb):
                    out_b[x0 : x0 + xn, y] = total[:, y * nz : (y + 1) * nz].reshape(xn, ch, nz)
        for b in held:
            store(b).start()
        return carry

    lax.fori_loop(0, steps, step, 0)
    for b in range(blocks):
        store(b).wait()


def lane(rows, wide):
    return lax.broadcasted_iota(jnp.int32, (rows, wide), 1)


def gather_partials(received, store, pencil, scale):
    modes = received.shape[1]
    for s in range(received.shape[0] // pencil):
        total = received[s * pencil].astype(F32)
        for p in range(1, pencil):
            total = total + received[s * pencil + p].astype(F32)
        store[s * modes : (s + 1) * modes, :] = (total * scale).astype(BF16).astype(F32)


def unpack(a, b):
    rows, wide = a.shape
    quarter = wide // (2 * HALVES)
    even = (lane(rows, wide) // quarter) % 2 == 0
    re = jnp.where(even, a, pltpu.roll(b, quarter, 1))
    im = jnp.where(even, pltpu.roll(a, wide - quarter, 1), b)
    return re, im


def pack(re, im):
    rows, wide = re.shape
    quarter = wide // (2 * HALVES)
    even = (lane(rows, wide) // quarter) % 2 == 0
    a = jnp.where(even, re, pltpu.roll(im, quarter, 1))
    b = jnp.where(even, pltpu.roll(re, wide - quarter, 1), im)
    return a, b


def swap(values):
    return pltpu.roll(values, values.shape[-1] // 2, 1)


def every(outer, inner, step):
    def body(o, carry):
        for i in range(inner):
            step(o, i)
        return carry

    lax.fori_loop(0, outer, body, 0)


def apply_kernel(got_a, got_b, weights, out_a, out_b, masked, ua, ub, va, vb, *, pencil, size, folded):
    outer, halves, kh, ch, wide = weights.shape
    samples = got_a.shape[0] // pencil
    total = got_a.shape[1]
    gather_partials(got_a, ua, pencil, 1.0)
    gather_partials(got_b, ub, pencil, 1.0)

    low = lane(samples, wide) < ch
    sign = jnp.where(low, -1.0, 1.0).astype(F32)
    zero = jnp.zeros((samples, wide), F32)

    def step(o, i):
        rows = pl.ds(o * kh + i, samples, stride=total)
        re, im = unpack(ua[rows, :], ub[rows, :])
        lhs = jnp.concatenate(
            [
                jnp.where(low, re, zero),
                jnp.where(low, im, zero),
                jnp.where(low, zero, re),
                jnp.where(low, zero, im),
            ],
            0,
        ).astype(BF16)
        masked[o * kh + i] = lhs
        rhs = jnp.concatenate([weights[o, 0, i], weights[o, 1, i]], 0)
        got = jnp.dot(lhs, rhs, preferred_element_type=F32)
        v0 = got[:samples] + sign * swap(got[samples : 2 * samples])
        v1 = got[2 * samples : 3 * samples] + sign * swap(got[3 * samples :])
        a, b = pack(jnp.where(low, v0, swap(v1)), jnp.where(low, swap(v0), v1))
        va[rows, :] = a
        vb[rows, :] = b

    every(outer, kh, step)
    scale = mode_scale(total, wide, kh, size, folded)
    for s in range(samples):
        for v, out in ((va, out_a), (vb, out_b)):
            value = (v[s * total : (s + 1) * total, :] * scale).astype(BF16)
            for p in range(pencil):
                out[s * pencil + p] = value


def mode_scale(modes, wide, kh, size, folded):
    first = lax.broadcasted_iota(jnp.int32, (modes, wide), 0) % kh == 0
    if not folded:
        first = first & (lane(modes, wide) < wide // HALVES)
    return jnp.where(first, 1.0 / size, 2.0 / size).astype(F32)


def adjoint_kernel(got_a, got_b, weights, out_a, out_b, stacked, ga, gb, va, vb, *, pencil, size, folded):
    outer, halves, kh, ch, wide = weights.shape
    samples = got_a.shape[0] // pencil
    total = got_a.shape[1]
    scale = 0.5 * mode_scale(total, wide, kh, size, folded)
    gather_partials(got_a, ga, pencil, scale)
    gather_partials(got_b, gb, pencil, scale)

    low = lane(samples, wide) < ch

    def step(o, i):
        rows = pl.ds(o * kh + i, samples, stride=total)
        re, im = unpack(ga[rows, :], gb[rows, :])
        er, mi = swap(re), swap(im)
        lhs = jnp.concatenate(
            [
                jnp.where(low, re, mi),
                jnp.where(low, im, -er),
                jnp.where(low, er, im),
                jnp.where(low, mi, -re),
            ],
            0,
        ).astype(BF16)
        stacked[o * kh + i] = lhs
        rhs = jnp.concatenate([weights[o, 0, i], weights[o, 1, i]], 0)
        got = lax.dot_general(
            lhs, rhs, (((1,), (1,)), ((), ())), preferred_element_type=F32
        )
        a, b = pack(
            jnp.where(low, got[:samples], got[2 * samples : 3 * samples]),
            jnp.where(low, got[samples : 2 * samples], got[3 * samples :]),
        )
        va[rows, :] = a
        vb[rows, :] = b

    every(outer, kh, step)
    for s in range(samples):
        for v, out in ((va, out_a), (vb, out_b)):
            value = v[s * total : (s + 1) * total, :].astype(BF16)
            for p in range(pencil):
                out[s * pencil + p] = value


def grads_kernel(masked, stacked, grad):
    kh, _, wide = masked.shape
    for i in range(kh):
        both = lax.dot_general(
            masked[i], stacked[i], (((0,), (0,)), ((), ())), preferred_element_type=F32
        )
        grad[0, 0, i] = both[: wide // 2]
        grad[0, 1, i] = both[wide // 2 :]


def params():
    return pltpu.CompilerParams(dimension_semantics=("arbitrary",), vmem_limit_bytes=LIMIT)


def whole(shape):
    return pl.BlockSpec(shape, lambda i, *r: (0,) * len(shape))


def make_body(dp, pencil):
    def body(field, cotangent, w_spec, w_local):
        sample = field[0]
        target = cotangent[0]
        xl, ny, ch, nz = sample.shape
        jo, lo, mz, _, wide = w_spec.shape
        nx, mx, my = xl * pencil, jo * dp, lo * pencil
        modes = my * mz
        folded = lo % HALVES == 0
        kh = mz if folded else mz // HALVES
        outer = jo * lo * mz // (HALVES * kh)
        hc = ch // HALVES
        owned = outer * kh
        size = nx * ny * nz
        xn = min(xl, 8)
        per = min(xl, 4)
        rank = lax.axis_index("pencil").astype(jnp.int32).reshape(1)

        xf, xi = kron_tables(nx, mx, pencil)
        ytab, ztab = grid_tables(ny, my, nz, mz, folded)
        weights = w_spec.reshape(outer, HALVES, kh, ch, wide)
        eye = jnp.eye(per, dtype=BF16)
        mix_out = [jnp.kron(eye, w_local[:, h * hc : (h + 1) * hc].T) for h in range(HALVES)]
        halved = w_local * jnp.asarray(0.5, BF16)
        mix_in = [jnp.kron(eye, halved[h * hc : (h + 1) * hc]) for h in range(HALVES)]

        def y_spec(yb):
            return whole(y_table(yb).shape)

        def y_table(yb):
            return ytab.reshape(2, HALVES, -1, yb, ytab.shape[-1])

        def held(yb, channels):
            return pltpu.VMEM((ny // yb, xl, yb, channels, nz), BF16)

        def sems(rows, yb):
            return pltpu.SemaphoreType.DMA((rows, ny // yb))

        z_spec = whole(ztab.shape)
        ranked = lambda t: pl.BlockSpec((1,) + t.shape[1:], lambda i, r: (r[0], 0, 0))
        anywhere = pl.BlockSpec(memory_space=pl.ANY)
        packed = (dp, pencil, jo, owned // jo, wide)
        flat = (dp * pencil, owned, wide)

        def call(kernel, yb, ins, outs, shapes, scratch, name, args, flops, alias=None):
            aliases = {}
            if alias is not None:
                ins = ins + [anywhere]
                args = args + (alias,)
                aliases = {len(args): 0}
            return pl.pallas_call(
                kernel,
                grid_spec=pltpu.PrefetchScalarGridSpec(
                    num_scalar_prefetch=1,
                    grid=(1,),
                    in_specs=ins,
                    out_specs=outs,
                    scratch_shapes=scratch,
                ),
                out_shape=shapes,
                input_output_aliases=aliases,
                compiler_params=params(),
                cost_estimate=pl.CostEstimate(
                    flops=flops, bytes_accessed=2 * sample.size, transcendentals=0
                ),
                name=name,
            )(rank, *args)

        def basis(yb):
            return [pltpu.VMEM((yb * nz, modes), BF16)] * HALVES

        acc = [pltpu.VMEM((xl, hc, modes), F32)] * HALVES
        turned = pltpu.VMEM((mx, wide, modes // HALVES), BF16)
        half = [pltpu.VMEM((xl, hc, modes), BF16)] * HALVES
        spectrum = jax.ShapeDtypeStruct(packed, BF16)
        grid_shape = jax.ShapeDtypeStruct(sample.shape, BF16)
        work = 2 * xl * hc * ny * nz * 2 * modes

        def exchange(values):
            return lax.all_to_all(values.reshape(flat), ("dp", "pencil"), 0, 0, tiled=True)

        def owner_call(kernel, args, ins, outs, shapes, scratch, name, steps=1):
            return pl.pallas_call(
                kernel,
                grid=(steps,),
                in_specs=ins,
                out_specs=outs,
                out_shape=shapes,
                scratch_shapes=scratch,
                compiler_params=params(),
                cost_estimate=pl.CostEstimate(
                    flops=work // 4, bytes_accessed=w_spec.size * 2, transcendentals=0
                ),
                name=name,
            )(*args)

        samples = dp
        moving = pl.BlockSpec((1, HALVES, kh, ch, wide), lambda i: (i, 0, 0, 0, 0))
        lines = pl.BlockSpec((kh, 4 * samples, wide), lambda i: (i, 0, 0))
        line_shape = jax.ShapeDtypeStruct((owned, 4 * samples, wide), BF16)
        message = jax.ShapeDtypeStruct(flat, BF16)
        store = pltpu.VMEM((samples * owned, wide), F32)
        options = dict(pencil=pencil, size=size, folded=folded)

        yb = 8
        got = []
        for h in range(HALVES):
            modes_h = call(
                functools.partial(forward_kernel, xn=xn, jo=jo, first=h * hc),
                yb,
                [anywhere, y_spec(yb), z_spec, ranked(xf)],
                whole(packed),
                spectrum,
                [*basis(yb), *acc, held(yb, hc), sems(1, yb)],
                "field_modes_%d" % h,
                (sample, y_table(yb), ztab, xf),
                work,
            )
            if got:
                modes_h, got[0] = lax.optimization_barrier((modes_h, got[0]))
            got.append(exchange(modes_h))
        va, vb, masked = owner_call(
            functools.partial(apply_kernel, **options),
            (got[0], got[1], weights),
            [whole(flat), whole(flat), whole(weights.shape)],
            (whole(flat), whole(flat), whole(line_shape.shape)),
            (message, message, line_shape),
            [store] * 4,
            "apply_modes",
        )
        spec = [exchange(va), exchange(vb)]
        yb = 4
        slope = None
        got = []
        for h in range(HALVES):
            slope, modes_h = call(
                functools.partial(slope_kernel, xn=xn, jo=jo, first=h * hc),
                yb,
                [
                    whole(flat),
                    whole(mix_out[h].shape),
                    y_spec(yb),
                    z_spec,
                    ranked(xf),
                    ranked(xi),
                    anywhere,
                    anywhere,
                ],
                (anywhere, whole(packed)),
                (grid_shape, spectrum),
                [*basis(yb), *acc, turned, *half, held(yb, ch), held(yb, hc), sems(3, yb)],
                "slope_modes_%d" % h,
                (spec[h], mix_out[h], y_table(yb), ztab, xf, xi, sample, target),
                3 * work,
                slope,
            )
            if got:
                modes_h, got[0] = lax.optimization_barrier((modes_h, got[0]))
            got.append(exchange(modes_h))
        da, db, stacked = owner_call(
            functools.partial(adjoint_kernel, **options),
            (got[0], got[1], weights),
            [whole(flat), whole(flat), whole(weights.shape)],
            (whole(flat), whole(flat), whole(line_shape.shape)),
            (message, message, line_shape),
            [store] * 4,
            "adjoint_modes",
        )
        spec = [exchange(da)]
        grad_w = owner_call(
            grads_kernel,
            (masked, stacked),
            [lines, lines],
            moving,
            jax.ShapeDtypeStruct(weights.shape, F32),
            [],
            "weight_grads",
            outer,
        )
        db, spec[0], grad_w, mix_in = lax.optimization_barrier((db, spec[0], grad_w, mix_in))
        spec.append(exchange(db))
        grad = None
        for h in range(HALVES):
            grad = call(
                functools.partial(inverse_kernel, xn=xn, jo=jo, pencil=pencil, first=h * hc),
                yb,
                [
                    whole(flat),
                    whole(mix_in[h].shape),
                    y_spec(yb),
                    z_spec,
                    ranked(xi),
                    anywhere,
                ],
                anywhere,
                grid_shape,
                [*basis(yb), turned, *half, held(yb, ch), held(yb, hc), sems(2, yb)],
                "grad_field_%d" % h,
                (spec[h], mix_in[h], y_table(yb), ztab, xi, slope),
                2 * work,
                grad,
            )
        return grad[None], grad_w.reshape(w_spec.shape)

    return body


def solution(mesh):
    split = P("dp", "pencil", None, None, None)
    return jax.shard_map(
        make_body(mesh.shape["dp"], mesh.shape["pencil"]),
        mesh=mesh,
        in_specs=(split, split, split, P()),
        out_specs=(split, split),
        check_vma=False,
    )
```

```python
import functools
import math

import jax
import jax.numpy as jnp
import numpy as np
from jax import lax
from jax.experimental import pallas as pl
from jax.experimental.pallas import tpu as pltpu
from jax.sharding import PartitionSpec as P

F32 = jnp.float32
BF16 = jnp.bfloat16
SUB = 16
LIMIT = 60 * 1024 * 1024
FIELD_ROWS = 4
BELL = 1.0 - 0.5 * math.log2(math.pi)


def phases(length, count, signed):
    position = np.arange(length)
    index = np.arange(count)
    freq = np.where(index < count // 2, index, index - count) if signed else index
    angle = np.mod(position[:, None] * freq[None, :], length) * (2.0 * math.pi / length)
    return np.cos(angle), np.sin(angle)


def kron_tables(nx, mx, parts):
    cos_x, sin_x = phases(nx, mx, True)
    eye = np.eye(SUB)
    local = nx // parts
    fwd, inv = [], []
    for p in range(parts):
        c = cos_x[p * local : (p + 1) * local]
        s = sin_x[p * local : (p + 1) * local]
        fwd.append(np.concatenate([np.kron(c.T, eye), np.kron(s.T, eye)], 1))
        inv.append(np.concatenate([np.kron(c, eye), np.kron(s, eye)], 1))
    return np.stack(fwd).astype(jnp.bfloat16), np.stack(inv).astype(jnp.bfloat16)


HALVES = 2


def grid_tables(ny, my, nz, mz, folded):
    cos_y, sin_y = phases(ny, my, True)
    cos_z, sin_z = phases(nz, mz, False)
    cos_z = cos_z.astype(jnp.bfloat16).astype(np.float32)
    sin_z = sin_z.astype(jnp.bfloat16).astype(np.float32)
    kh = mz // HALVES

    def pick(y, z, t):
        if folded:
            y = y[: ny // HALVES, t::HALVES]
        else:
            z = z[:, t * kh : (t + 1) * kh]
        return np.repeat(y, z.shape[1], 1), np.tile(z, (1, y.shape[1]))

    ytab, ztab = [], []
    for y, z in ((cos_y, cos_z), (sin_y, sin_z)):
        pairs = [pick(y, z, t) for t in range(HALVES)]
        ytab.append([p[0] for p in pairs])
        ztab.append([p[1] for p in pairs])
    return np.array(ytab, np.float32), np.array(ztab, np.float32)


def fill_basis(basis, ytab, ztab, i):
    yb = ytab.shape[3]
    nz = ztab.shape[2]
    for t in range(HALVES):
        cz = ztab[0, t]
        sz = ztab[1, t]
        for y in range(yb):
            cy = ytab[0, t, i, y : y + 1, :]
            sy = ytab[1, t, i, y : y + 1, :]
            re = cy * cz - sy * sz
            im = -(sy * cz + cy * sz)
            basis[t][y * nz : (y + 1) * nz, :] = jnp.concatenate([re, im], 1).astype(BF16)


def x_forward_store(acc, xf, out, mx):
    xl, ch, wide = acc[0].shape
    kept = wide // 2
    parts = []
    for g in range(ch // SUB):
        sides = []
        for t in range(HALVES):
            a = acc[t][:, g * SUB : (g + 1) * SUB, :].reshape(xl * SUB, wide).astype(BF16)
            re = a[:, :kept]
            im = a[:, kept:]
            sides.append(
                jnp.concatenate(
                    [jnp.concatenate([re, im], 1), jnp.concatenate([im, -re], 1)], 0
                )
            )
        rhs = jnp.concatenate(sides, 1)
        parts.append(jnp.dot(xf, rhs, preferred_element_type=F32))
    dp, pencil, jo, mo, _ = out.shape
    for j in range(mx):
        rows = slice(j * SUB, (j + 1) * SUB)
        pieces = [
            part[rows, n * kept : (n + 1) * kept] for n in range(2 * HALVES) for part in parts
        ]
        turned = jnp.concatenate(pieces, 0).T.astype(BF16)
        for q in range(pencil):
            out[j // jo, q, j % jo] = turned[q * mo : (q + 1) * mo, :]


def x_inverse_load(spec, turned, xi, half, jo, pencil):
    xl, ch, wide = half[0].shape
    mx = turned.shape[0]
    mo = spec.shape[1] // jo
    for j in range(mx):
        first = (j // jo) * pencil
        rows = slice((j % jo) * mo, (j % jo + 1) * mo)
        block = jnp.concatenate([spec[first + q, rows] for q in range(pencil)], 0)
        turned[j] = block.astype(F32).T.astype(BF16)
    for g in range(ch // SUB):
        sides = []
        for t in range(HALVES):
            re, im = [
                turned[:, n * ch + g * SUB : n * ch + (g + 1) * SUB, :].reshape(
                    mx * SUB, wide // 2
                )
                for n in (2 * t, 2 * t + 1)
            ]
            sides.append(
                jnp.concatenate(
                    [jnp.concatenate([re, im], 1), jnp.concatenate([-im, re], 1)], 0
                )
            )
        b = jnp.dot(xi, jnp.concatenate(sides, 1), preferred_element_type=F32)
        for t in range(HALVES):
            half[t][:, g * SUB : (g + 1) * SUB, :] = (
                b[:, t * wide : (t + 1) * wide].reshape(xl, SUB, wide).astype(BF16)
            )


def grid_rows(ref, x0, xn, yb):
    ch, nz = ref.shape[2], ref.shape[3]
    return jnp.concatenate(
        [ref[x0 : x0 + xn, y].reshape(xn * ch, nz) for y in range(yb)], 1
    )


def mixed(mix, ref, x0, xn, yb):
    per = mix.shape[1] // ref.shape[2]
    table = mix[...]
    return jnp.concatenate(
        [
            jnp.dot(table, grid_rows(ref, x, per, yb), preferred_element_type=F32)
            for x in range(x0, x0 + xn, per)
        ],
        0,
    )


def forward_sums(values, basis, acc, x0, xn):
    ch = acc[0].shape[1]
    if len(values) == 2:
        sides = (values[0] + values[1], values[0] - values[1])
    else:
        sides = (values[0], values[0])
    for t in range(HALVES):
        part = jnp.dot(sides[t], basis[t][...], preferred_element_type=F32)
        acc[t][x0 : x0 + xn] += part.reshape(xn, ch, part.shape[1])


def inverse_sums(half, basis, x0, xn, count):
    sides = []
    for t in range(HALVES):
        rows = half[t][x0 : x0 + xn]
        rows = rows.reshape(xn * rows.shape[1], rows.shape[2])
        sides.append(
            lax.dot_general(
                rows, basis[t][...], (((1,), (1,)), ((), ())), preferred_element_type=F32
            )
        )
    if count == 2:
        return [sides[0] + sides[1], sides[0] - sides[1]]
    return [sides[0] + sides[1]]


def block_copies(src, dst, sems, row, first):
    _, _, yb, chans, _ = dst.shape

    def one(i):
        return pltpu.make_async_copy(
            src.at[:, pl.ds(i * yb, yb), pl.ds(first, chans)], dst.at[i], sems.at[row, i]
        )

    return one


def step_blocks(i, steps, blocks):
    return [i + n * steps for n in range(blocks // steps)]


AHEAD = 2


def start_first(steps, blocks, loads):
    for i in range(min(AHEAD, steps)):
        for b in step_blocks(i, steps, blocks):
            for load in loads:
                load(b).start()


def start_next(i, steps, blocks, loads):
    @pl.when(i + AHEAD < steps)
    def _():
        for b in step_blocks(i + AHEAD, steps, blocks):
            for load in loads:
                load(b).start()


def forward_kernel(rank, field, ytab, ztab, xf, out, b0, b1, *rest, xn, jo):
    basis = (b0, b1)
    fbuf, sems = rest[-2:]
    acc = [rest[h * HALVES : (h + 1) * HALVES] for h in range(HALVES)]
    _, blocks, xl, yb, ch, nz = fbuf.shape
    steps = ytab.shape[2]
    loads = [block_copies(field, fbuf.at[h], sems, h, h * ch) for h in range(HALVES)]
    start_first(steps, blocks, loads)
    for part in rest[: HALVES * HALVES]:
        part[...] = jnp.zeros_like(part)

    def step(i, carry):
        fill_basis(basis, ytab, ztab, i)
        held = step_blocks(i, steps, blocks)
        start_next(i, steps, blocks, loads)
        for h in range(HALVES):
            for b in held:
                loads[h](b).wait()
            for x0 in range(0, xl, xn):
                values = [grid_rows(fbuf.at[h, b], x0, xn, yb) for b in held]
                forward_sums(values, basis, acc[h], x0, xn)
        return carry

    lax.fori_loop(0, steps, step, 0)
    for h in range(HALVES):
        x_forward_store(acc[h], xf[0], out.at[:, :, h], xf.shape[1] // SUB)


def slope_kernel(rank, spec, mix, ytab, ztab, xf, xi, field, cot, *rest, xn, jo, first):
    slope, out, b0, b1, a0, a1, turned, h0, h1, fbuf, cbuf, sems = rest[-12:]
    basis, acc, half = (b0, b1), (a0, a1), (h0, h1)
    blocks, xl, yb, ch, nz = cbuf.shape
    steps = ytab.shape[2]
    load_f = block_copies(field, fbuf, sems, 0, 0)
    load_c = block_copies(cot, cbuf, sems, 1, first)
    start_first(steps, blocks, [load_f, load_c])

    def store(b):
        return pltpu.make_async_copy(
            cbuf.at[b], slope.at[:, pl.ds(b * yb, yb), pl.ds(first, ch)], sems.at[2, b]
        )

    for part in acc:
        part[...] = jnp.zeros_like(part)
    x_inverse_load(spec, turned, xi[0], half, jo, out.shape[1])

    def step(i, carry):
        fill_basis(basis, ytab, ztab, i)
        held = step_blocks(i, steps, blocks)
        start_next(i, steps, blocks, [load_f, load_c])
        for b in held:
            load_f(b).wait()
            load_c(b).wait()
        starts = list(range(0, xl, xn))

        def before(x0):
            grid = inverse_sums(half, basis, x0, xn, len(held))
            return [
                pre + mixed(mix, fbuf.at[b], x0, xn, yb) for b, pre in zip(held, grid)
            ]

        ahead = before(starts[0])
        for n, x0 in enumerate(starts):
            grid = ahead
            if n + 1 < len(starts):
                ahead = before(starts[n + 1])
            values = []
            for b, pre in zip(held, grid):
                cot_b = cbuf.at[b]
                q = pre * (1.0 / math.sqrt(2.0))
                bell = jnp.exp2(q * q * (-math.log2(math.e)) + BELL) * q
                gain = (1.0 + lax.erf(q)) + bell
                value = grid_rows(cot_b, x0, xn, yb) * gain.astype(BF16)
                for y in range(yb):
                    cot_b[x0 : x0 + xn, y] = value[:, y * nz : (y + 1) * nz].reshape(xn, ch, nz)
                values.append(value)
            forward_sums(values, basis, acc, x0, xn)
        for b in held:
            store(b).start()
        return carry

    lax.fori_loop(0, steps, step, 0)
    x_forward_store(acc, xf[0], out, xf.shape[1] // SUB)
    for b in range(blocks):
        store(b).wait()


def inverse_kernel(rank, spec, mix, ytab, ztab, xi, slope, *rest, xn, jo, pencil, first):
    grad, b0, b1, turned, h0, h1, sbuf, gbuf, sems = rest[-9:]
    basis, half = (b0, b1), (h0, h1)
    blocks, xl, yb, ch, nz = gbuf.shape
    steps = ytab.shape[2]
    load = block_copies(slope, sbuf, sems, 0, 0)
    start_first(steps, blocks, [load])

    def store(b):
        return pltpu.make_async_copy(
            gbuf.at[b], grad.at[:, pl.ds(b * yb, yb), pl.ds(first, ch)], sems.at[1, b]
        )

    x_inverse_load(spec, turned, xi[0], half, jo, pencil)

    def step(i, carry):
        fill_basis(basis, ytab, ztab, i)
        held = step_blocks(i, steps, blocks)
        start_next(i, steps, blocks, [load])
        for b in held:
            load(b).wait()
        starts = list(range(0, xl, xn))

        def before(x0):
            grid = inverse_sums(half, basis, x0, xn, len(held))
            return [(mixed(mix, sbuf.at[b], x0, xn, yb), g) for b, g in zip(held, grid)]

        ahead = before(starts[0])
        for n, x0 in enumerate(starts):
            grid = ahead
            if n + 1 < len(starts):
                ahead = before(starts[n + 1])
            for b, (spread, total) in zip(held, grid):
                out_b = gbuf.at[b]
                total = (total + spread).astype(BF16)
                for y in range(yb):
                    out_b[x0 : x0 + xn, y] = total[:, y * nz : (y + 1) * nz].reshape(xn, ch, nz)
        for b in held:
            store(b).start()
        return carry

    lax.fori_loop(0, steps, step, 0)
    for b in range(blocks):
        store(b).wait()


def lane(rows, wide):
    return lax.broadcasted_iota(jnp.int32, (rows, wide), 1)


def gather_partials(received, store, pencil, scale):
    modes = received.shape[1]
    for s in range(received.shape[0] // pencil):
        total = received[s * pencil].astype(F32)
        for p in range(1, pencil):
            total = total + received[s * pencil + p].astype(F32)
        store[s * modes : (s + 1) * modes, :] = (total * scale).astype(BF16).astype(F32)


def unpack(a, b):
    rows, wide = a.shape
    quarter = wide // (2 * HALVES)
    even = (lane(rows, wide) // quarter) % 2 == 0
    re = jnp.where(even, a, pltpu.roll(b, quarter, 1))
    im = jnp.where(even, pltpu.roll(a, wide - quarter, 1), b)
    return re, im


def pack(re, im):
    rows, wide = re.shape
    quarter = wide // (2 * HALVES)
    even = (lane(rows, wide) // quarter) % 2 == 0
    a = jnp.where(even, re, pltpu.roll(im, quarter, 1))
    b = jnp.where(even, pltpu.roll(re, wide - quarter, 1), im)
    return a, b


def swap(values):
    return pltpu.roll(values, values.shape[-1] // 2, 1)


def every(outer, inner, step):
    def body(o, carry):
        for i in range(inner):
            step(o, i)
        return carry

    lax.fori_loop(0, outer, body, 0)


def apply_kernel(
    got, weights, out_a, out_b, masked, ua, ub, va, vb, *, pencil, size, folded
):
    outer, halves, kh, ch, wide = weights.shape
    samples = got.shape[0] // pencil
    total = outer * kh
    got_a = got.at[:, pl.ds(0, total)]
    got_b = got.at[:, pl.ds(total, total)]
    gather_partials(got_a, ua, pencil, 1.0)
    gather_partials(got_b, ub, pencil, 1.0)

    low = lane(samples, wide) < ch
    sign = jnp.where(low, -1.0, 1.0).astype(F32)
    zero = jnp.zeros((samples, wide), F32)

    def step(o, i):
        rows = pl.ds(o * kh + i, samples, stride=total)
        re, im = unpack(ua[rows, :], ub[rows, :])
        lhs = jnp.concatenate(
            [
                jnp.where(low, re, zero),
                jnp.where(low, im, zero),
                jnp.where(low, zero, re),
                jnp.where(low, zero, im),
            ],
            0,
        ).astype(BF16)
        masked[o * kh + i] = lhs
        rhs = jnp.concatenate([weights[o, 0, i], weights[o, 1, i]], 0)
        got = jnp.dot(lhs, rhs, preferred_element_type=F32)
        v0 = got[:samples] + sign * swap(got[samples : 2 * samples])
        v1 = got[2 * samples : 3 * samples] + sign * swap(got[3 * samples :])
        a, b = pack(jnp.where(low, v0, swap(v1)), jnp.where(low, swap(v0), v1))
        va[rows, :] = a
        vb[rows, :] = b

    every(outer, kh, step)
    scale = mode_scale(total, wide, kh, size, folded)
    for s in range(samples):
        for v, out in ((va, out_a), (vb, out_b)):
            value = (v[s * total : (s + 1) * total, :] * scale).astype(BF16)
            for p in range(pencil):
                out[s * pencil + p] = value


def mode_scale(modes, wide, kh, size, folded):
    first = lax.broadcasted_iota(jnp.int32, (modes, wide), 0) % kh == 0
    if not folded:
        first = first & (lane(modes, wide) < wide // HALVES)
    return jnp.where(first, 1.0 / size, 2.0 / size).astype(F32)


def adjoint_kernel(got_a, got_b, weights, out_a, out_b, stacked, ga, gb, va, vb, *, pencil, size, folded):
    outer, halves, kh, ch, wide = weights.shape
    samples = got_a.shape[0] // pencil
    total = got_a.shape[1]
    scale = 0.5 * mode_scale(total, wide, kh, size, folded)
    gather_partials(got_a, ga, pencil, scale)
    gather_partials(got_b, gb, pencil, scale)

    low = lane(samples, wide) < ch

    def step(o, i):
        rows = pl.ds(o * kh + i, samples, stride=total)
        re, im = unpack(ga[rows, :], gb[rows, :])
        er, mi = swap(re), swap(im)
        lhs = jnp.concatenate(
            [
                jnp.where(low, re, mi),
                jnp.where(low, im, -er),
                jnp.where(low, er, im),
                jnp.where(low, mi, -re),
            ],
            0,
        ).astype(BF16)
        stacked[o * kh + i] = lhs
        rhs = jnp.concatenate([weights[o, 0, i], weights[o, 1, i]], 0)
        got = lax.dot_general(
            lhs, rhs, (((1,), (1,)), ((), ())), preferred_element_type=F32
        )
        a, b = pack(
            jnp.where(low, got[:samples], got[2 * samples : 3 * samples]),
            jnp.where(low, got[samples : 2 * samples], got[3 * samples :]),
        )
        va[rows, :] = a
        vb[rows, :] = b

    every(outer, kh, step)
    for s in range(samples):
        for v, out in ((va, out_a), (vb, out_b)):
            value = v[s * total : (s + 1) * total, :].astype(BF16)
            for p in range(pencil):
                out[s * pencil + p] = value


def grads_kernel(masked, stacked, grad):
    kh, _, wide = masked.shape
    for i in range(kh):
        both = lax.dot_general(
            masked[i], stacked[i], (((0,), (0,)), ((), ())), preferred_element_type=F32
        )
        grad[0, 0, i] = both[: wide // 2]
        grad[0, 1, i] = both[wide // 2 :]


def params():
    return pltpu.CompilerParams(dimension_semantics=("arbitrary",), vmem_limit_bytes=LIMIT)


def whole(shape):
    return pl.BlockSpec(shape, lambda i, *r: (0,) * len(shape))


def make_body(dp, pencil):
    def body(field, cotangent, w_spec, w_local):
        sample = field[0]
        target = cotangent[0]
        xl, ny, ch, nz = sample.shape
        jo, lo, mz, _, wide = w_spec.shape
        nx, mx, my = xl * pencil, jo * dp, lo * pencil
        modes = my * mz
        folded = lo % HALVES == 0
        kh = mz if folded else mz // HALVES
        outer = jo * lo * mz // (HALVES * kh)
        hc = ch // HALVES
        owned = outer * kh
        size = nx * ny * nz
        xn = min(xl, 8)
        per = min(xl, 4)
        rank = lax.axis_index("pencil").astype(jnp.int32).reshape(1)

        xf, xi = kron_tables(nx, mx, pencil)
        ytab, ztab = grid_tables(ny, my, nz, mz, folded)
        weights = w_spec.reshape(outer, HALVES, kh, ch, wide)
        eye = jnp.eye(per, dtype=BF16)
        mix_out = [jnp.kron(eye, w_local[:, h * hc : (h + 1) * hc].T) for h in range(HALVES)]
        halved = w_local * jnp.asarray(0.5, BF16)
        mix_in = [jnp.kron(eye, halved[h * hc : (h + 1) * hc]) for h in range(HALVES)]

        def y_spec(yb):
            return whole(y_table(yb).shape)

        def y_table(yb):
            return ytab.reshape(2, HALVES, -1, yb, ytab.shape[-1])

        def held(yb, channels):
            return pltpu.VMEM((ny // yb, xl, yb, channels, nz), BF16)

        def sems(rows, yb):
            return pltpu.SemaphoreType.DMA((rows, ny // yb))

        z_spec = whole(ztab.shape)
        ranked = lambda t: pl.BlockSpec((1,) + t.shape[1:], lambda i, r: (r[0], 0, 0))
        anywhere = pl.BlockSpec(memory_space=pl.ANY)
        packed = (dp, pencil, jo, owned // jo, wide)
        flat = (dp * pencil, owned, wide)

        def call(kernel, yb, ins, outs, shapes, scratch, name, args, flops, alias=None):
            aliases = {}
            if alias is not None:
                ins = ins + [anywhere]
                args = args + (alias,)
                aliases = {len(args): 0}
            return pl.pallas_call(
                kernel,
                grid_spec=pltpu.PrefetchScalarGridSpec(
                    num_scalar_prefetch=1,
                    grid=(1,),
                    in_specs=ins,
                    out_specs=outs,
                    scratch_shapes=scratch,
                ),
                out_shape=shapes,
                input_output_aliases=aliases,
                compiler_params=params(),
                cost_estimate=pl.CostEstimate(
                    flops=flops, bytes_accessed=2 * sample.size, transcendentals=0
                ),
                name=name,
            )(rank, *args)

        def basis(yb):
            return [pltpu.VMEM((yb * nz, modes), BF16)] * HALVES

        acc = [pltpu.VMEM((xl, hc, modes), F32)] * HALVES
        turned = pltpu.VMEM((mx, wide, modes // HALVES), BF16)
        half = [pltpu.VMEM((xl, hc, modes), BF16)] * HALVES
        spectrum = jax.ShapeDtypeStruct(packed, BF16)
        grid_shape = jax.ShapeDtypeStruct(sample.shape, BF16)
        work = 2 * xl * hc * ny * nz * 2 * modes

        def exchange(values):
            return lax.all_to_all(values.reshape(flat), ("dp", "pencil"), 0, 0, tiled=True)

        def owner_call(kernel, args, ins, outs, shapes, scratch, name, steps=1):
            return pl.pallas_call(
                kernel,
                grid=(steps,),
                in_specs=ins,
                out_specs=outs,
                out_shape=shapes,
                scratch_shapes=scratch,
                compiler_params=params(),
                cost_estimate=pl.CostEstimate(
                    flops=work // 4, bytes_accessed=w_spec.size * 2, transcendentals=0
                ),
                name=name,
            )(*args)

        samples = dp
        moving = pl.BlockSpec((1, HALVES, kh, ch, wide), lambda i: (i, 0, 0, 0, 0))
        lines = pl.BlockSpec((kh, 4 * samples, wide), lambda i: (i, 0, 0))
        line_shape = jax.ShapeDtypeStruct((owned, 4 * samples, wide), BF16)
        message = jax.ShapeDtypeStruct(flat, BF16)
        store = pltpu.VMEM((samples * owned, wide), F32)
        options = dict(pencil=pencil, size=size, folded=folded)

        yb = FIELD_ROWS
        both = packed[:2] + (HALVES,) + packed[2:]
        sent = call(
            functools.partial(forward_kernel, xn=xn, jo=jo),
            yb,
            [anywhere, y_spec(yb), z_spec, ranked(xf)],
            whole(both),
            jax.ShapeDtypeStruct(both, BF16),
            [
                *basis(yb),
                *acc,
                *acc,
                pltpu.VMEM((HALVES, ny // yb, xl, yb, hc, nz), BF16),
                sems(HALVES, yb),
            ],
            "field_modes",
            (sample, y_table(yb), ztab, xf),
            2 * work,
        )
        paired = (dp * pencil, HALVES * owned, wide)
        got = lax.all_to_all(sent.reshape(paired), ("dp", "pencil"), 0, 0, tiled=True)
        va, vb, masked = owner_call(
            functools.partial(apply_kernel, **options),
            (got, weights),
            [whole(paired), whole(weights.shape)],
            (whole(flat), whole(flat), whole(line_shape.shape)),
            (message, message, line_shape),
            [store] * 4,
            "apply_modes",
        )
        spec = [exchange(va), exchange(vb)]
        yb = 4
        slope = None
        got = []
        for h in range(HALVES):
            slope, modes_h = call(
                functools.partial(slope_kernel, xn=xn, jo=jo, first=h * hc),
                yb,
                [
                    whole(flat),
                    whole(mix_out[h].shape),
                    y_spec(yb),
                    z_spec,
                    ranked(xf),
                    ranked(xi),
                    anywhere,
                    anywhere,
                ],
                (anywhere, whole(packed)),
                (grid_shape, spectrum),
                [*basis(yb), *acc, turned, *half, held(yb, ch), held(yb, hc), sems(3, yb)],
                "slope_modes_%d" % h,
                (spec[h], mix_out[h], y_table(yb), ztab, xf, xi, sample, target),
                3 * work,
                slope,
            )
            if got:
                modes_h, got[0] = lax.optimization_barrier((modes_h, got[0]))
            got.append(exchange(modes_h))
        da, db, stacked = owner_call(
            functools.partial(adjoint_kernel, **options),
            (got[0], got[1], weights),
            [whole(flat), whole(flat), whole(weights.shape)],
            (whole(flat), whole(flat), whole(line_shape.shape)),
            (message, message, line_shape),
            [store] * 4,
            "adjoint_modes",
        )
        spec = [exchange(da)]
        grad_w = owner_call(
            grads_kernel,
            (masked, stacked),
            [lines, lines],
            moving,
            jax.ShapeDtypeStruct(weights.shape, F32),
            [],
            "weight_grads",
            outer,
        )
        db, spec[0], grad_w, mix_in = lax.optimization_barrier((db, spec[0], grad_w, mix_in))
        spec.append(exchange(db))
        grad = None
        for h in range(HALVES):
            grad = call(
                functools.partial(inverse_kernel, xn=xn, jo=jo, pencil=pencil, first=h * hc),
                yb,
                [
                    whole(flat),
                    whole(mix_in[h].shape),
                    y_spec(yb),
                    z_spec,
                    ranked(xi),
                    anywhere,
                ],
                anywhere,
                grid_shape,
                [*basis(yb), turned, *half, held(yb, ch), held(yb, hc), sems(2, yb)],
                "grad_field_%d" % h,
                (spec[h], mix_in[h], y_table(yb), ztab, xi, slope),
                2 * work,
                grad,
            )
        return grad[None], grad_w.reshape(w_spec.shape)

    return body


def solution(mesh):
    split = P("dp", "pencil", None, None, None)
    return jax.shard_map(
        make_body(mesh.shape["dp"], mesh.shape["pencil"]),
        mesh=mesh,
        in_specs=(split, split, split, P()),
        out_specs=(split, split),
        check_vma=False,
    )
```
